32 devices in a mesh: dp: 4 (over y, x), expert: 8 (over z, core).
Axes of the slice: x: 2, y: 2, z: 4, core: 2. Of those that a mesh axis runs over, the one named last changes fastest.
Arguments:
- tokens: bfloat16 [4096, 4096], P(('dp', 'expert')), may hold values from -6 to 6
- gate_proj: bfloat16 [8, 768, 4096], P('expert', 'dp'), may hold values from -0.09375 to 0.09375
- up_proj: bfloat16 [8, 768, 4096], P('expert', 'dp'), may hold values from -0.09375 to 0.09375
- down_proj: bfloat16 [8, 768, 4096], P('expert', 'dp'), may hold values from -0.21875 to 0.21875
- route_ids: int32 [4096, 2], P(('dp', 'expert')), may hold values from 0 to 7, as said below
- route_slots: int32 [4096, 2], P(('dp', 'expert')), may hold values from 0 to 95, as said below
- route_gates: float32 [4096, 2], P(('dp', 'expert')), may hold values from 0.1 to 1
- image_shard: int32 [4, 8], P(None, 'expert'), may hold values from 0 to 3, as said below
- norm_gain: float32 [4096], replicated, may hold values from 0.5 to 1.5
- key_proj: bfloat16 [4096, 1024], P('dp'), may hold values from -0.09375 to 0.09375
Outputs:
- student_rows: bfloat16 [4096, 4096], P(('dp', 'expert'))
- keys: bfloat16 [4096, 1024], P(('dp', 'expert'))
The draws below stay inside these ranges and needn't reach their ends.
Inputs may be any that keep to these rules, and one draw needn't show every extreme that they name: `route_ids`: within the rows of one device a token names 2 different experts and no expert is named more than 2 * 48 times; on every device some expert is named exactly 2 * 48 times. `route_slots`: within the rows of one device the mentions of one expert carry the numbers 0 up to their count minus one, each once; one expert has 48 retained mentions from every device. `image_shard`: for each e, of the 4 image tiles of column e exactly 1 name each shard.
All inputs are finite; a program needn't handle non-finite values.
Results may differ from the reference program's by a relative error of at most 0.007.
Values may be sent and summed in bfloat16 or wider, within the bound.
A program may use at most 128 MiB of HBM per device.

```python
import math
import jax
import jax.numpy as jnp
from jax import lax

D = 4096
EFF = 768
KV_WIDTH = 1024
TOPK = 2
IMG_TOK = 128
TOK_DEV = 128
EXPERTS = 8
CAP = 48
IMG_DEV = 1
TOKENS = 4096
N_DP = 4
N_EXPERT = 8


def route_table(key):
    block_count = TOKENS // TOK_DEV
    queue_depth = 2 * CAP
    cell_count = EXPERTS * queue_depth
    tickets = TOK_DEV * TOPK
    liking = 1 + jax.random.randint(jax.random.fold_in(key, 11), (EXPERTS, 1), 0, 4)
    favored = jax.random.randint(jax.random.fold_in(key, 12), (), 0, EXPERTS)
    expert_of = jnp.arange(cell_count, dtype=jnp.int32) // queue_depth

    def one_block(position):
        block_key = jax.random.fold_in(jax.random.fold_in(key, 13), position)
        busiest = jax.random.randint(jax.random.fold_in(block_key, 1), (), 0, EXPERTS)
        base_score = jax.random.randint(jax.random.fold_in(block_key, 2), (EXPERTS, queue_depth), 0, 65536)
        base_score = (base_score * liking).reshape(-1)
        forced = (expert_of == favored) | (expert_of == busiest)
        ranking = jnp.where(forced, 262144, base_score) * cell_count + jnp.arange(cell_count, dtype=jnp.int32)
        chosen = jnp.sort(lax.top_k(ranking, tickets)[1].astype(jnp.int32))
        chosen_experts = chosen // queue_depth
        before = jnp.sum((chosen_experts[None, :] < chosen_experts[:, None]).astype(jnp.int32), axis=1)
        queue_slots = jnp.arange(tickets, dtype=jnp.int32) - before
        layout_ids = chosen_experts.reshape(TOPK, TOK_DEV).T
        layout_slots = queue_slots.reshape(TOPK, TOK_DEV).T
        shuffle = jax.random.permutation(jax.random.fold_in(block_key, 3), TOK_DEV)
        return (layout_ids[shuffle], layout_slots[shuffle])
    all_ids, all_slots = jax.vmap(one_block)(jnp.arange(block_count, dtype=jnp.int32))
    return (all_ids.reshape(TOKENS, TOPK).astype(jnp.int32), all_slots.reshape(TOKENS, TOPK).astype(jnp.int32))


def draw_route_ids(key, part):
    return route_table(key)[0]


def draw_route_slots(key, part):
    return route_table(key)[1]


def draw_image_shard(key, part):
    images_col = N_DP * IMG_DEV

    def column(position):
        column_key = jax.random.fold_in(jax.random.fold_in(key, 21), position)
        return jax.random.permutation(column_key, images_col).astype(jnp.int32) // IMG_DEV
    layout = jax.vmap(column)(jnp.arange(N_EXPERT, dtype=jnp.int32))
    return layout.reshape(N_EXPERT, N_DP, IMG_DEV).transpose(1, 0, 2).reshape(N_DP, N_EXPERT * IMG_DEV)


def block_levels(own_key, extent, split, smallest, high):
    gain, own = 1.0, jax.random.fold_in(own_key, 6)
    for dim, blocks in split:
        heights = jnp.exp(jax.random.uniform(jax.random.fold_in(own, dim), (blocks,), jnp.float32, smallest / len(split), high / len(split)))
        gain = gain * jnp.repeat(heights, extent[dim] // blocks).reshape([-1 if axis == dim else 1 for axis in range(len(extent))])
    return gain


def centred(stream_key, shape, deviation, reach, pieces=(), held_as=jnp.bfloat16):
    entries = deviation * jax.random.normal(stream_key, shape, jnp.float32)
    if pieces:
        entries = entries * block_levels(stream_key, shape, pieces, -0.22, 0.18)
    return jnp.clip(entries, -reach, reach).astype(held_as)


def setup_inputs(seed: int = 0) -> dict:
    streams_of = jax.random.split(jax.random.key(seed), 11)
    return {
        "tokens": centred(streams_of[0], (TOKENS, D), 1.0, 6.0, ((0, 32),)),
        "gate_proj": centred(streams_of[1], (EXPERTS, EFF, D), D ** -0.5, 0.09375, ((0, 8), (1, 4))),
        "up_proj": centred(streams_of[2], (EXPERTS, EFF, D), D ** -0.5, 0.09375, ((0, 8), (1, 4))),
        "down_proj": centred(streams_of[3], (EXPERTS, EFF, D), EFF ** -0.5, 0.21875, ((0, 8), (1, 4))),
        "route_ids": draw_route_ids(jax.random.fold_in(streams_of[10], 71), 0),
        "route_slots": draw_route_slots(jax.random.fold_in(streams_of[10], 71), 0),
        "route_gates": jnp.clip(jnp.exp(math.log(1.0) - 2.3025851 * jax.random.uniform(streams_of[6], (TOKENS, TOPK), jnp.float32) ** block_levels(streams_of[6], (TOKENS, TOPK), ((0, 32),), -0.2, 0.2)), 0.1, 1.0),
        "image_shard": draw_image_shard(jax.random.fold_in(streams_of[10], 71), 0),
        "norm_gain": jnp.clip(1.0 + 0.1 * jax.random.normal(streams_of[8], (D,), jnp.float32), 0.5, 1.5),
        "key_proj": centred(streams_of[9], (D, KV_WIDTH), D ** -0.5, 0.09375, ((0, 4),)),
    }


def normalize(values, norm_gain):
    wide = values.astype(jnp.float32)
    mean_square = lax.optimization_barrier(jnp.mean(wide * wide, axis=-1, keepdims=True))
    return (wide * lax.rsqrt(mean_square + 1e-05) * norm_gain).astype(jnp.bfloat16)

def reference(tokens, gate_proj, up_proj, down_proj, route_ids, route_slots, route_gates, image_shard, norm_gain, key_proj):
    block_count = N_DP * N_EXPERT
    slot_total = EXPERTS * CAP
    blocks = tokens.reshape(block_count, TOK_DEV, D)
    choice_ids = route_ids.reshape(block_count, TOK_DEV * TOPK)
    choice_slots = route_slots.reshape(block_count, TOK_DEV * TOPK)
    choice_gates = route_gates.reshape(block_count, TOK_DEV * TOPK)
    retained = choice_slots < CAP
    slot_cells = jnp.where(retained, choice_ids * CAP + choice_slots, slot_total).astype(jnp.int32)
    owners = jnp.arange(TOK_DEV * TOPK, dtype=jnp.int32) // TOPK

    def fill_tokens(cell_row):
        return jnp.full((slot_total + 1,), TOK_DEV, jnp.int32).at[cell_row].set(owners)[:slot_total]

    def fill_gates(cell_row, gate_row):
        return jnp.zeros((slot_total + 1,), jnp.float32).at[cell_row].set(gate_row.astype(jnp.float32))[:slot_total]
    cell_token = jax.vmap(fill_tokens)(slot_cells).reshape(block_count, EXPERTS, CAP)
    cell_gate = jax.vmap(fill_gates)(slot_cells, choice_gates).reshape(block_count, EXPERTS, CAP)

    def take_rows(block, senders):
        return jnp.take(block, senders, axis=0, mode='fill', fill_value=0)

    def add_rows(running, senders, contribution):
        return running.at[senders].add(contribution, mode='drop')

    def expert_step(accumulated, expert):
        senders = lax.dynamic_index_in_dim(cell_token, expert, 1, keepdims=False)
        weights_now = lax.dynamic_index_in_dim(cell_gate, expert, 1, keepdims=False)
        gathered = jax.vmap(take_rows)(blocks, senders).reshape(block_count * CAP, D)
        gate_rows = lax.dynamic_index_in_dim(gate_proj, expert, 0, keepdims=False)
        up_rows = lax.dynamic_index_in_dim(up_proj, expert, 0, keepdims=False)
        down_rows = lax.dynamic_index_in_dim(down_proj, expert, 0, keepdims=False)
        dims = (((1,), (1,)), ((), ()))
        gate_act = lax.dot_general(gathered, gate_rows, dims, preferred_element_type=jnp.float32)
        up_act = lax.dot_general(gathered, up_rows, dims, preferred_element_type=jnp.float32)
        hidden = (jax.nn.silu(gate_act) * up_act).astype(jnp.bfloat16)
        result = jnp.dot(hidden, down_rows, preferred_element_type=jnp.float32).astype(jnp.bfloat16)
        result = result.reshape(block_count, CAP, D)
        contribution = weights_now[:, :, None] * result.astype(jnp.float32)
        accumulated = jax.vmap(add_rows)(accumulated, senders, contribution)
        return (accumulated, None)
    accumulated, unused = lax.scan(expert_step, blocks.astype(jnp.float32), jnp.arange(EXPERTS, dtype=jnp.int32))
    teacher = accumulated.astype(jnp.bfloat16)
    images_col = N_DP * IMG_DEV
    arranged = teacher.reshape(N_DP, N_EXPERT, IMG_DEV, IMG_TOK, D).transpose(1, 0, 2, 3, 4)
    arranged = arranged.reshape(N_EXPERT, images_col, IMG_TOK, D)
    targets = image_shard.reshape(N_DP, N_EXPERT, IMG_DEV).transpose(1, 0, 2).reshape(N_EXPERT, images_col)
    order_key = targets * images_col + jnp.arange(images_col, dtype=jnp.int32)[None, :]
    arrangement = jnp.argsort(order_key, axis=1).astype(jnp.int32)

    def pick_images(column_rows, column_order):
        return jnp.take(column_rows, column_order, axis=0)
    relaid = jax.vmap(pick_images)(arranged, arrangement)
    student_rows = relaid.reshape(N_EXPERT, N_DP, IMG_DEV, IMG_TOK, D).transpose(1, 0, 2, 3, 4).reshape(TOKENS, D)
    normed = normalize(student_rows, norm_gain)
    keys = jnp.dot(normed, key_proj, preferred_element_type=jnp.float32).astype(jnp.bfloat16)
    return (student_rows, keys)
```

```python
import functools

import jax
import jax.numpy as jnp
from jax import lax
from jax.experimental import pallas as pl
from jax.experimental.pallas import tpu as pltpu
from jax.sharding import PartitionSpec as P

IMG_TOK = 128


def normalize(values, norm_gain):
    wide = values.astype(jnp.float32)
    mean_square = jnp.mean(wide * wide, axis=-1, keepdims=True)
    return (wide * lax.rsqrt(mean_square + 1e-05) * norm_gain).astype(jnp.bfloat16)


def activate(incoming, gate_rows, up_rows):
    dims = (((1,), (1,)), ((), ()))
    gate_act = lax.dot_general(incoming, gate_rows, dims, preferred_element_type=jnp.float32)
    up_act = lax.dot_general(incoming, up_rows, dims, preferred_element_type=jnp.float32)
    return (jax.nn.silu(gate_act) * up_act).astype(jnp.bfloat16)


CHUNKS = 4
PIECES = 2
GROUP = 16
MESH = pl.DeviceIdType.MESH


def fused_kernel(
    n_expert,
    capacity,
    ids_ref,
    slots_ref,
    gates_ref,
    shard_ref,
    gain_ref,
    tokens_ref,
    gate_ref,
    up_ref,
    down_ref,
    key_ref,
    student_ref,
    keys_ref,
    gate_buf,
    up_buf,
    down_buf,
    key_buf,
    outgoing,
    incoming,
    produced,
    returned,
    tiles,
    passed,
    far,
    tok_half,
    hidden,
    gained,
    mixing,
    acc_keys,
    acc_gate,
    acc_up,
    squares,
    send_sem,
    recv_sem,
    spare_send,
    spare_recv,
    local_sem,
):
    d = lax.axis_index("dp")
    e = lax.axis_index("expert")
    dx = d + 1 - 2 * (d % 2)
    dy = (d + 2) % 4
    dd = (dx + 2) % 4
    core = e % 2
    sibling = e + 1 - 2 * core
    w = dx + core * (dy - dx)
    t = dy + core * (dx - dy)
    tok_dev, width = tokens_ref.shape
    units = gate_ref.shape[1]
    half = width // 2
    quarter_width = width // 4
    chunk = half // CHUNKS
    per_quarter = CHUNKS // 2
    key_rows, key_width = key_ref.shape
    key_half = key_rows // 2
    piece = key_half // PIECES
    half_piece = piece // 2
    slots = n_expert * capacity
    groups = capacity // GROUP
    block = n_expert * GROUP
    counts = {"remote": 0, "local": 0}
    sent = []

    def send(source, target, where):
        index = counts["remote"]
        counts["remote"] += 1
        copy = pltpu.make_async_remote_copy(
            src_ref=source,
            dst_ref=target,
            send_sem=send_sem.at[index],
            recv_sem=recv_sem.at[index],
            device_id=where,
            device_id_type=MESH,
        )
        copy.start()
        sent.append(copy)
        return copy

    def local(source, target):
        index = counts["local"]
        counts["local"] += 1
        copy = pltpu.make_async_copy(source, target, local_sem.at[index])
        copy.start()
        return copy

    to_x, to_y, to_sibling = {"dp": dx}, {"dp": dy}, {"expert": sibling}
    to_w, to_t, to_d = {"dp": w}, {"dp": t}, {"dp": dd}
    hops = range(1, n_expert)
    peers = {k: lax.rem(e + k, n_expert) for k in hops}
    senders = {k: lax.rem(e + n_expert - k, n_expert) for k in hops}

    def quarter_of(owner, p):
        return (owner // 2) * 2 + p

    def unit_rows(owner):
        place = owner % 2 + core * (owner // 2 - owner % 2)
        return pl.ds(pl.multiple_of(place * units, units), units)

    def quarter_cols(owner, p):
        return pl.ds(pl.multiple_of(quarter_of(owner, p) * quarter_width, quarter_width), quarter_width)

    def chunk_cols(owner, c):
        first = quarter_of(owner, c // per_quarter) * quarter_width + (c % per_quarter) * chunk
        return pl.ds(pl.multiple_of(first, chunk), chunk)

    def group_rows(g, who):
        return pl.ds(pl.multiple_of(g * block + who * GROUP, GROUP), GROUP)

    def incoming_rows(g, s, who):
        return pl.ds(pl.multiple_of((g * 2 + s) * block + who * GROUP, GROUP), GROUP)

    barrier = pltpu.get_barrier_semaphore()
    for where in [to_x, to_y, to_d] + [{"expert": peers[k]} for k in hops]:
        pl.semaphore_signal(barrier, inc=1, device_id=where, device_id_type=MESH)
    pl.semaphore_wait(barrier, n_expert + 2)

    mine = unit_rows(d)
    gate_w = send(gate_ref.at[0], gate_buf.at[mine, :], to_w)
    up_w = send(up_ref.at[0], up_buf.at[mine, :], to_w)
    down_x, down_y, down_f, own_down = [], [], [], []
    for p in range(2):
        cols = pl.ds(p * quarter_width, quarter_width)
        down_y.append(
            send(down_ref.at[0, :, quarter_cols(dy, p)], down_buf.at[1 - core, mine, cols], to_y)
        )
    own_gate = local(gate_ref.at[0], gate_buf.at[mine, :])
    own_up = local(up_ref.at[0], up_buf.at[mine, :])
    for p in range(2):
        cols = pl.ds(p * quarter_width, quarter_width)
        down_x.append(send(down_ref.at[0, :, quarter_cols(d, p)], down_buf.at[core, mine, cols], to_x))
        own_down.append(local(down_ref.at[0, :, quarter_cols(d, p)], down_buf.at[0, mine, cols]))
    own_key = local(key_ref, key_buf.at[d])

    step = 512
    grid = lax.broadcasted_iota(jnp.int32, (slots, tok_dev), 0)
    mix = jnp.zeros((slots, tok_dev), jnp.float32)
    named = jnp.zeros((slots, tok_dev), jnp.float32)
    for k in range(ids_ref.shape[0]):
        queue = slots_ref[k : k + 1, :]
        place = lax.div(queue, GROUP) * block + ids_ref[k : k + 1, :] * GROUP + lax.rem(queue, GROUP)
        cell = jnp.where(queue < capacity, place, slots)
        hit = grid == cell
        mix += jnp.where(hit, gates_ref[k : k + 1, :], 0.0)
        named += jnp.where(hit, 1.0, 0.0)
    spread = named.astype(jnp.bfloat16)

    dispatched, forwarded = [], []
    for g in range(groups):
        chosen = spread[g * block : (g + 1) * block, :]

        def fill(i, carry):
            cols = pl.ds(pl.multiple_of(i * step, step), step)
            rows = jnp.dot(chosen, tokens_ref[:, cols], preferred_element_type=jnp.float32)
            outgoing[pl.ds(g * block, block), cols] = rows.astype(jnp.bfloat16)
            return carry

        lax.fori_loop(0, width // step, fill, 0)
        dispatched.append(
            {
                k: send(
                    outgoing.at[group_rows(g, peers[k]), :],
                    incoming.at[incoming_rows(g, 0, e), :],
                    {"expert": peers[k]},
                )
                for k in hops
            }
        )
        forwarded.append(
            [send(outgoing.at[group_rows(g, e), :], incoming.at[incoming_rows(g, 1, e), :], to_t)]
        )
        incoming[incoming_rows(g, 0, e), :] = outgoing[group_rows(g, e), :]

    turned = mix.T
    mix_hi = turned.astype(jnp.bfloat16)
    mixing[0, 0] = mix_hi
    mixing[0, 1] = (turned - mix_hi.astype(jnp.float32)).astype(jnp.bfloat16)

    def forward(g):
        for k in hops:
            dispatched[g][k].wait_recv()
            forwarded[g].append(
                send(
                    incoming.at[incoming_rows(g, 0, senders[k]), :],
                    incoming.at[incoming_rows(g, 1, senders[k]), :],
                    to_t,
                )
            )

    dims = (((1,), (1,)), ((), ()))
    deep = 1024
    handed, spares = [], []

    def activate(g):
        for copy in forwarded[g]:
            copy.wait_recv()
        here = pl.ds(g * 2 * block, 2 * block)
        acc_gate[...] = jnp.zeros_like(acc_gate)
        acc_up[...] = jnp.zeros_like(acc_up)

        def add(i, carry):
            cols = pl.ds(pl.multiple_of(i * deep, deep), deep)
            rows = incoming[here, cols]
            acc_gate[...] += lax.dot_general(
                rows, gate_buf[:, cols], dims, preferred_element_type=jnp.float32
            )
            acc_up[...] += lax.dot_general(
                rows, up_buf[:, cols], dims, preferred_element_type=jnp.float32
            )
            return carry

        lax.fori_loop(0, width // deep, add, 0)
        gate_act = acc_gate[...]
        act = (gate_act / (1.0 + jnp.exp(-gate_act)) * acc_up[...]).astype(jnp.bfloat16)
        at = pl.ds(g * block, block)
        hidden[0, at, :] = act[:block]
        hidden[1 + 3 * core, at, :] = act[block:]
        handed.append(
            [
                send(hidden.at[0, at, :], hidden.at[3 - 2 * core, at, :], to_y),
                send(hidden.at[1 + 3 * core, at, :], hidden.at[2, at, :], to_t),
            ]
        )
        spare = pltpu.make_async_remote_copy(
            src_ref=hidden.at[4, at, :],
            dst_ref=hidden.at[3, at, :],
            send_sem=spare_send.at[g],
            recv_sem=spare_recv.at[g],
            device_id=to_d,
            device_id_type=MESH,
        )
        spares.append(spare)

        @pl.when(core == 1)
        def _():
            spare.start()

    hands = []

    def give(g, cols):
        for s in range(2):
            returned[s, group_rows(g, e), cols] = produced[g * 2 + s, pl.ds(pl.multiple_of(e * GROUP, GROUP), GROUP), cols]
        return [
            send(
                produced.at[pl.ds(g * 2, 2), pl.ds(pl.multiple_of(peers[k] * GROUP, GROUP), GROUP), cols],
                returned.at[:, group_rows(g, e), cols],
                {"expert": peers[k]},
            )
            for k in hops
        ]

    def project(g, first, count):
        here = pl.ds(g * block, block)

        def one(i, carry):
            at = pl.ds(pl.multiple_of(i * chunk, chunk), chunk)
            total = jnp.zeros((2 * block, chunk), jnp.float32)
            for pair in range(2):
                acts = hidden[pl.ds(2 * pair, 2), here, :].reshape(2 * block, 2 * units)
                total += jnp.dot(acts, down_buf[pair, :, at], preferred_element_type=jnp.float32)
            rows = total.astype(jnp.bfloat16)
            produced[g * 2, :, at] = rows[:block]
            produced[g * 2 + 1, :, at] = rows[block:]
            return carry

        lax.fori_loop(first, first + count, one, 0)

    def key_rows_at(owner, p, start=0, size=piece):
        first = (owner % 2) * key_half + p * piece + start
        return pl.ds(pl.multiple_of(first, half_piece), size)

    key_first, key_second, key_shared = [], [], []

    def key_own(p):
        rows = key_rows_at(e, p)
        part = key_ref.at[rows, :]
        place = key_buf.at[d, rows, :]
        key_first.append((send(part, place, to_x), send(part, place, to_y)))

    def pass_key(owner, rows, where):
        part = key_buf.at[owner, rows, :]
        return send(part, part, where)

    def key_share(owner, rows):
        key_shared.append(pass_key(owner, rows, to_sibling))

    def key_middle(p):
        key_x, key_y = key_first[p]
        rows = key_rows_at(e, p)
        key_y.wait_recv()
        d0 = pass_key(dy, key_rows_at(e, p, 0, half_piece), to_x)
        key_x.wait_recv()
        d1 = pass_key(dx, key_rows_at(e, p, half_piece, half_piece), to_y)
        key_second.append((d0, d1))
        key_share(dy, rows)
        key_share(dx, rows)

    def key_diagonal(p):
        d0, d1 = key_second[p]
        d0.wait_recv()
        key_share(dd, key_rows_at(e, p, 0, half_piece))
        d1.wait_recv()
        key_share(dd, key_rows_at(e, p, half_piece, half_piece))

    def collect(g):
        for copy in handed[g]:
            copy.wait_recv()

        @pl.when(core == 1)
        def _():
            spares[g].wait_recv()

    acc_keys[...] = jnp.zeros_like(acc_keys)
    squares[...] = jnp.zeros_like(squares)
    owners = (d, dy, dx, dd)
    tile_w, tile_t = [], []

    def flag(owner, shard):
        return jnp.where(shard_ref[owner] == shard, 1.0, 0.0)

    def combine(c):
        for copy in hands[groups - 1 + c]:
            copy.wait_recv()
        cols = pl.ds(c * chunk, chunk)
        for s in range(2):
            rows = returned[s, :, cols]
            branch = jnp.dot(mixing[s, 0], rows, preferred_element_type=jnp.float32)
            branch += jnp.dot(mixing[s, 1], rows, preferred_element_type=jnp.float32)
            base = tokens_ref[:, chunk_cols(d, c)] if s == 0 else tok_half[:, cols]
            tiles[s, :, cols] = (base.astype(jnp.float32) + branch).astype(jnp.bfloat16)
        tile_w.append(send(tiles.at[pl.ds(0, 2), :, cols], tiles.at[pl.ds(2, 2), :, cols], to_x))

    def keep(rows, at):
        student_ref[:, at] = rows.astype(jnp.bfloat16)
        gained[:, at] = (rows * gain_ref[:, at]).astype(jnp.bfloat16)
        squares[...] += jnp.sum(rows * rows, axis=-1, keepdims=True)

    def swap(c):
        tile_w[c].wait_recv()
        cols = pl.ds(c * chunk, chunk)
        stay = jnp.zeros((tok_dev, chunk), jnp.float32)
        leave = jnp.zeros((tok_dev, chunk), jnp.float32)
        for slot in range(4):
            rows = tiles[slot, :, cols].astype(jnp.float32)
            stay += flag(owners[slot], d) * rows
            leave += flag(owners[slot], dy) * rows
        passed[:, cols] = leave.astype(jnp.bfloat16)
        tile_t.append(send(passed.at[:, cols], far.at[:, cols], to_y))
        keep(stay, chunk_cols(d, c))

    def finish(c):
        tile_t[c].wait_recv()
        keep(far[:, pl.ds(c * chunk, chunk)].astype(jnp.float32), chunk_cols(dy, c))

    def keys_of(owner, c):
        q = quarter_of(owner, c // per_quarter)
        acc_keys[...] += jnp.dot(
            gained[:, chunk_cols(owner, c)],
            key_buf[q, pl.ds((c % per_quarter) * chunk, chunk), :],
            preferred_element_type=jnp.float32,
        )

    forward(0)
    for p in range(2):
        cols = pl.ds(p * quarter_width, quarter_width)
        down_y[p].wait_recv()
        part = down_buf.at[1 - core, unit_rows(dy), cols]
        down_f.append(send(part, down_buf.at[1, unit_rows(dy), cols], to_x))
    forward(1)
    for copy in (own_gate, own_up):
        copy.wait()
    for copy in (gate_w, up_w):
        copy.wait_recv()
    activate(0)
    for g in range(1, groups - 1):
        activate(g)
    for g in range(2, groups):
        forward(g)
    others = [send(mixing.at[0], mixing.at[1], to_y)]
    for p in range(2):
        cols = pl.ds(p * quarter_width, quarter_width)
        others.append(send(tokens_ref.at[:, quarter_cols(dy, p)], tok_half.at[:, cols], to_y))
    for copy in own_down:
        copy.wait()
    for copy in down_x + down_f:
        copy.wait_recv()
    every = pl.ds(0, half)
    for g in range(groups):
        if g == 1:
            activate(groups - 1)
            for p in range(PIECES):
                key_own(p)
        collect(g)
        if g < groups - 1:
            project(g, 0, CHUNKS)
            hands.append(give(g, every))
        else:
            for c in range(CHUNKS):
                project(g, c, 1)
                hands.append(give(g, pl.ds(c * chunk, chunk)))
    for p in range(PIECES):
        key_middle(p)
    for p in range(PIECES):
        key_diagonal(p)
    for copy in others:
        copy.wait_recv()
    for g in range(groups - 1):
        for copy in hands[g]:
            copy.wait_recv()
    own_key.wait()
    for c in range(CHUNKS + 2):
        if c < CHUNKS:
            combine(c)
        if 0 <= c - 1 < CHUNKS:
            swap(c - 1)
        if c == 1:
            for copy in key_shared:
                copy.wait_recv()
        if 0 <= c - 1 < CHUNKS:
            keys_of(d, c - 1)
        if 0 <= c - 2 < CHUNKS:
            finish(c - 2)
            keys_of(dy, c - 2)
    scale = lax.rsqrt(squares[...] / width + 1e-05)
    keys_ref[...] = (acc_keys[...] * scale).astype(jnp.bfloat16)
    for copy in sent:
        copy.wait_send()

    @pl.when(core == 1)
    def _():
        for copy in spares:
            copy.wait_send()


def fused(
    tokens,
    gate_proj,
    up_proj,
    down_proj,
    route_ids,
    route_slots,
    route_gates,
    image_shard,
    norm_gain,
    key_proj,
    capacity,
):
    tok_dev, width = tokens.shape
    n_expert = lax.axis_size("expert")
    slots = n_expert * capacity
    groups = capacity // GROUP
    units = gate_proj.shape[1]
    half_width = width // 2
    key_rows, key_width = key_proj.shape
    remote = 8 + 8 * PIECES + (n_expert - 1) * (2 * groups + groups - 1 + CHUNKS) + 3 * groups + 3 + 2 * CHUNKS
    vmem = pl.BlockSpec(memory_space=pltpu.VMEM)
    anywhere = pl.BlockSpec(memory_space=pl.ANY)
    scalars = pl.BlockSpec(memory_space=pltpu.SMEM)
    half = jnp.bfloat16
    return pl.pallas_call(
        functools.partial(fused_kernel, n_expert, capacity),
        out_shape=(
            jax.ShapeDtypeStruct((tok_dev, width), half),
            jax.ShapeDtypeStruct((tok_dev, key_width), half),
        ),
        in_specs=[vmem] * 3 + [scalars] + [vmem] * 2 + [anywhere] * 4,
        out_specs=(vmem, vmem),
        scratch_shapes=[
            pltpu.VMEM((2 * units, width), half),
            pltpu.VMEM((2 * units, width), half),
            pltpu.VMEM((2, 2 * units, half_width), half),
            pltpu.VMEM((4, key_rows, key_width), half),
            pltpu.VMEM((slots, width), half),
            pltpu.VMEM((2 * slots, width), half),
            pltpu.VMEM((2 * groups, n_expert * GROUP, half_width), half),
            pltpu.VMEM((2, slots, half_width), half),
            pltpu.VMEM((4, tok_dev, half_width), half),
            pltpu.VMEM((tok_dev, half_width), half),
            pltpu.VMEM((tok_dev, half_width), half),
            pltpu.VMEM((tok_dev, half_width), half),
            pltpu.VMEM((5, slots, 2 * units), half),
            pltpu.VMEM((tok_dev, width), half),
            pltpu.VMEM((2, 2, tok_dev, slots), half),
            pltpu.VMEM((tok_dev, key_width), jnp.float32),
            pltpu.VMEM((2 * n_expert * GROUP, 2 * units), jnp.float32),
            pltpu.VMEM((2 * n_expert * GROUP, 2 * units), jnp.float32),
            pltpu.VMEM((tok_dev, 1), jnp.float32),
            pltpu.SemaphoreType.DMA((remote,)),
            pltpu.SemaphoreType.DMA((remote,)),
            pltpu.SemaphoreType.DMA((groups,)),
            pltpu.SemaphoreType.DMA((groups,)),
            pltpu.SemaphoreType.DMA((5,)),
        ],
        compiler_params=pltpu.CompilerParams(
            collective_id=0, has_side_effects=True, vmem_limit_bytes=60 * 1024 * 1024
        ),
    )(
        route_ids.T,
        route_slots.T,
        route_gates.T,
        image_shard.reshape(-1),
        norm_gain.reshape(1, -1),
        tokens,
        gate_proj,
        up_proj,
        down_proj,
        key_proj,
    )


def per_device(
    tokens,
    gate_proj,
    up_proj,
    down_proj,
    route_ids,
    route_slots,
    route_gates,
    image_shard,
    norm_gain,
    key_proj,
):
    tok_dev, model_width = tokens.shape
    top_count = route_ids.shape[1]
    experts = gate_proj.shape[0] * lax.axis_size("expert")
    capacity = 3 * tok_dev * top_count // (2 * experts)
    if capacity % 16 == 0 and gate_proj.shape[0] == 1 and lax.axis_size("dp") == 4 and experts % 2 == 0:
        if tok_dev == IMG_TOK and gate_proj.shape[1] % 64 == 0 and key_proj.shape[0] % 512 == 0:
            return fused(
                tokens,
                gate_proj,
                up_proj,
                down_proj,
                route_ids,
                route_slots,
                route_gates,
                image_shard,
                norm_gain,
                key_proj,
                capacity,
            )
    slot_total = experts * capacity
    retained = route_slots < capacity
    slot_cells = jnp.where(retained, route_ids * capacity + route_slots, slot_total).reshape(-1)
    owners = jnp.arange(tok_dev * top_count, dtype=jnp.int32) // top_count
    cell_token = (
        jnp.full((slot_total + 1,), tok_dev, jnp.int32).at[slot_cells].set(owners)[:slot_total]
    )
    outgoing = jnp.take(tokens, cell_token, axis=0, mode="fill", fill_value=0).reshape(
        experts, capacity, model_width
    )
    arrived = lax.all_to_all(outgoing, "expert", split_axis=0, concat_axis=0, tiled=True)
    incoming = arrived.reshape(-1, model_width)
    hidden = activate(
        incoming,
        lax.all_gather(gate_proj, "dp", axis=1, tiled=True)[0],
        lax.all_gather(up_proj, "dp", axis=1, tiled=True)[0],
    )
    summed = jnp.dot(
        hidden,
        lax.all_gather(down_proj, "dp", axis=1, tiled=True)[0],
        preferred_element_type=jnp.float32,
    )
    produced = summed.astype(jnp.bfloat16).reshape(arrived.shape)
    returned = lax.all_to_all(produced, "expert", split_axis=0, concat_axis=0, tiled=True).reshape(
        -1, model_width
    )
    picked = jnp.take(returned, slot_cells, axis=0, mode="fill", fill_value=0).reshape(
        tok_dev, top_count, model_width
    )
    mixing = jnp.where(retained, route_gates, 0.0)
    branch = jnp.einsum("tk,tkd->td", mixing, picked.astype(jnp.float32))
    teacher = (tokens.astype(jnp.float32) + branch).astype(jnp.bfloat16)
    gathered = lax.all_gather(teacher, "dp", axis=0, tiled=True)
    shard_column = image_shard.reshape(-1)
    images_col = shard_column.shape[0]
    arrangement = jnp.argsort(shard_column * images_col + jnp.arange(images_col, dtype=jnp.int32))
    images = gathered.reshape(images_col, IMG_TOK, model_width)
    position = lax.axis_index("dp")
    ordered = jnp.take(images, arrangement, axis=0).reshape(images_col * IMG_TOK, model_width)
    student_rows = lax.dynamic_slice_in_dim(ordered, position * tok_dev, tok_dev, 0)
    normed = normalize(ordered, norm_gain)
    columns = lax.dynamic_slice_in_dim(normed, position * key_proj.shape[0], key_proj.shape[0], 1)
    projected = lax.psum_scatter(
        jnp.dot(columns, key_proj, preferred_element_type=jnp.float32),
        "dp",
        scatter_dimension=0,
        tiled=True,
    )
    return (student_rows, projected.astype(jnp.bfloat16))


def solution(mesh):
    in_specs = (
        P(("dp", "expert"), None),
        P("expert", "dp", None),
        P("expert", "dp", None),
        P("expert", "dp", None),
        P(("dp", "expert"), None),
        P(("dp", "expert"), None),
        P(("dp", "expert"), None),
        P(None, "expert"),
        P(),
        P("dp", None),
    )
    out_specs = (P(("dp", "expert"), None), P(("dp", "expert"), None))
    return jax.shard_map(
        per_device, mesh=mesh, in_specs=in_specs, out_specs=out_specs, check_vma=False
    )
```

```python
import functools

import jax
import jax.numpy as jnp
from jax import lax
from jax.experimental import pallas as pl
from jax.experimental.pallas import tpu as pltpu
from jax.sharding import PartitionSpec as P

IMG_TOK = 128


def normalize(values, norm_gain):
    wide = values.astype(jnp.float32)
    mean_square = jnp.mean(wide * wide, axis=-1, keepdims=True)
    return (wide * lax.rsqrt(mean_square + 1e-05) * norm_gain).astype(jnp.bfloat16)


def activate(incoming, gate_rows, up_rows):
    dims = (((1,), (1,)), ((), ()))
    gate_act = lax.dot_general(incoming, gate_rows, dims, preferred_element_type=jnp.float32)
    up_act = lax.dot_general(incoming, up_rows, dims, preferred_element_type=jnp.float32)
    return (jax.nn.silu(gate_act) * up_act).astype(jnp.bfloat16)


CHUNKS = 4
ORDER = (
    "G", "w0", "w1", "|", "F0", "W", "t0", "t1", "A0", "O0", "O1", "F1", "C0", "P00", "F2", "P01", "A1", "C1", "P13", "P10", "A2", "T", "K", "C2", "L1",
)
GROUP = 16
MESH = pl.DeviceIdType.MESH


def fused_kernel(
    n_expert,
    capacity,
    ids_ref,
    slots_ref,
    gates_ref,
    shard_ref,
    gain_ref,
    tokens_ref,
    gate_ref,
    up_ref,
    down_ref,
    key_ref,
    student_ref,
    keys_ref,
    gate_buf,
    up_buf,
    down_buf,
    key_buf,
    outgoing,
    incoming,
    produced,
    returned,
    tiles,
    passed,
    far,
    tok_half,
    hidden,
    gained,
    mixing,
    far_ids,
    far_slots,
    far_gates,
    key_part,
    acc_keys,
    acc_gate,
    acc_up,
    squares,
    send_sem,
    recv_sem,
    spare_send,
    spare_recv,
    local_sem,
):
    d = lax.axis_index("dp")
    e = lax.axis_index("expert")
    dx = d + 1 - 2 * (d % 2)
    dy = (d + 2) % 4
    dd = (dx + 2) % 4
    core = e % 2
    sibling = e + 1 - 2 * core
    w = dx + core * (dy - dx)
    t = dy + core * (dx - dy)
    tok_dev, width = tokens_ref.shape
    units = gate_ref.shape[1]
    half = width // 2
    quarter_width = width // 4
    chunk = half // CHUNKS
    per_quarter = CHUNKS // 2
    key_rows, key_width = key_ref.shape
    key_piece = key_rows // 4
    slots = n_expert * capacity
    groups = capacity // GROUP
    block = n_expert * GROUP
    counts = {"remote": 0, "local": 0}
    sent = []

    def send(source, target, where, go=True):
        index = counts["remote"]
        counts["remote"] += 1
        copy = pltpu.make_async_remote_copy(
            src_ref=source,
            dst_ref=target,
            send_sem=send_sem.at[index],
            recv_sem=recv_sem.at[index],
            device_id=where,
            device_id_type=MESH,
        )
        if go:
            copy.start()
        sent.append(copy)
        return copy

    def local(source, target):
        index = counts["local"]
        counts["local"] += 1
        copy = pltpu.make_async_copy(source, target, local_sem.at[index])
        copy.start()
        return copy

    to_x, to_y, to_sibling = {"dp": dx}, {"dp": dy}, {"expert": sibling}
    to_w, to_t, to_d = {"dp": w}, {"dp": t}, {"dp": dd}
    hops = range(1, n_expert)
    peers = {k: lax.rem(e + k, n_expert) for k in hops}
    senders = {k: lax.rem(e + n_expert - k, n_expert) for k in hops}

    def quarter_of(owner, p):
        return (owner // 2) * 2 + p

    def unit_rows(owner):
        place = owner % 2 + core * (owner // 2 - owner % 2)
        return pl.ds(pl.multiple_of(place * units, units), units)

    def quarter_cols(owner, p):
        return pl.ds(pl.multiple_of(quarter_of(owner, p) * quarter_width, quarter_width), quarter_width)

    def chunk_cols(owner, c):
        first = quarter_of(owner, c // per_quarter) * quarter_width + (c % per_quarter) * chunk
        return pl.ds(pl.multiple_of(first, chunk), chunk)

    def group_rows(g, who):
        return pl.ds(pl.multiple_of(g * block + who * GROUP, GROUP), GROUP)

    def incoming_rows(g, s, who):
        return pl.ds(pl.multiple_of((g * 2 + s) * block + who * GROUP, GROUP), GROUP)

    barrier = pltpu.get_barrier_semaphore()
    for where in [to_x, to_y, to_d] + [{"expert": peers[k]} for k in hops]:
        pl.semaphore_signal(barrier, inc=1, device_id=where, device_id_type=MESH)

    step = 512

    def routes(ids, queues):
        grid = lax.broadcasted_iota(jnp.int32, (slots, tok_dev), 0)
        hits = []
        for k in range(ids.shape[0]):
            queue = queues[k : k + 1, :]
            place = lax.div(queue, GROUP) * block + ids[k : k + 1, :] * GROUP + lax.rem(queue, GROUP)
            hits.append(grid == jnp.where(queue < capacity, place, slots))
        return hits

    def mix_into(s, ids, queues, weights):
        mix = jnp.zeros((slots, tok_dev), jnp.float32)
        for k, hit in enumerate(routes(ids, queues)):
            mix += jnp.where(hit, weights[k : k + 1, :], 0.0)
        turned = mix.T
        mix_hi = turned.astype(jnp.bfloat16)
        mixing[s, 0] = mix_hi
        mixing[s, 1] = (turned - mix_hi.astype(jnp.float32)).astype(jnp.bfloat16)

    named = jnp.zeros((slots, tok_dev), jnp.float32)
    for hit in routes(ids_ref, slots_ref):
        named += jnp.where(hit, 1.0, 0.0)
    spread = named.astype(jnp.bfloat16)

    def fill_group(g):
        chosen = spread[g * block : (g + 1) * block, :]

        def fill(i, carry):
            cols = pl.ds(pl.multiple_of(i * step, step), step)
            rows = jnp.dot(chosen, tokens_ref[:, cols], preferred_element_type=jnp.float32)
            outgoing[pl.ds(g * block, block), cols] = rows.astype(jnp.bfloat16)
            return carry

        lax.fori_loop(0, width // step, fill, 0)

    fill_group(0)
    pl.semaphore_wait(barrier, n_expert + 2)

    mine = unit_rows(d)
    down_x, down_y, down_f, own_down = [], [], [], []

    def half_cols(p):
        return pl.ds(p * quarter_width, quarter_width)

    for p in range(2):
        part = down_ref.at[0, :, quarter_cols(dy, p)]
        down_y.append(send(part, down_buf.at[1 - core, mine, half_cols(p)], to_y, False))
        part = down_ref.at[0, :, quarter_cols(d, p)]
        down_x.append(send(part, down_buf.at[core, mine, half_cols(p)], to_x, False))

    def down_to_y(p):
        down_y[p].start()

    def down_to_x(p):
        down_x[p].start()

    def down_to_w(p):
        @pl.when(core == 0)
        def _():
            down_x[p].start()

        @pl.when(core == 1)
        def _():
            down_y[p].start()

    def down_to_t(p):
        @pl.when(core == 0)
        def _():
            down_y[p].start()

        @pl.when(core == 1)
        def _():
            down_x[p].start()

    def down_on(p):
        down_y[p].wait_recv()
        part = down_buf.at[1 - core, unit_rows(dy), half_cols(p)]
        down_f.append(send(part, down_buf.at[1, unit_rows(dy), half_cols(p)], to_x))

    def down_here(p):
        own_down[p].wait()
        down_x[p].wait_recv()
        down_f[p].wait_recv()

    pulled = []

    def pull():
        pulled.append(send(gate_ref.at[0], gate_buf.at[mine, :], to_w))
        pulled.append(send(up_ref.at[0], up_buf.at[mine, :], to_w))

    def pulled_in():
        own_gate.wait()
        own_up.wait()
        for copy in pulled:
            copy.wait_recv()

    own_gate = local(gate_ref.at[0], gate_buf.at[mine, :])
    own_up = local(up_ref.at[0], up_buf.at[mine, :])
    for p in range(2):
        own_down.append(local(down_ref.at[0, :, quarter_cols(d, p)], down_buf.at[0, mine, half_cols(p)]))
    own_key = local(key_ref, key_buf.at[d % 2])

    for token in ORDER[: ORDER.index("|")]:
        {"G": pull, "Y": down_to_y, "X": down_to_x, "w": down_to_w, "t": down_to_t}[token[0]](*[int(i) for i in token[1:]])
    dispatched, forwarded = [], []
    for g in range(groups):
        if g:
            fill_group(g)
        dispatched.append(
            {
                k: send(
                    outgoing.at[group_rows(g, peers[k]), :],
                    incoming.at[incoming_rows(g, 0, e), :],
                    {"expert": peers[k]},
                )
                for k in hops
            }
        )
        forwarded.append(
            [send(outgoing.at[group_rows(g, e), :], incoming.at[incoming_rows(g, 1, e), :], to_t)]
        )
        incoming[incoming_rows(g, 0, e), :] = outgoing[group_rows(g, e), :]

    mix_into(0, ids_ref, slots_ref, gates_ref)

    def forward(g):
        for k in hops:
            dispatched[g][k].wait_recv()
            forwarded[g].append(
                send(
                    incoming.at[incoming_rows(g, 0, senders[k]), :],
                    incoming.at[incoming_rows(g, 1, senders[k]), :],
                    to_t,
                )
            )

    dims = (((1,), (1,)), ((), ()))
    deep = 1024
    handed, spares = [], []

    def activate(g):
        for copy in forwarded[g]:
            copy.wait_recv()
        here = pl.ds(g * 2 * block, 2 * block)
        acc_gate[...] = jnp.zeros_like(acc_gate)
        acc_up[...] = jnp.zeros_like(acc_up)

        def add(i, carry):
            cols = pl.ds(pl.multiple_of(i * deep, deep), deep)
            rows = incoming[here, cols]
            acc_gate[...] += lax.dot_general(
                rows, gate_buf[:, cols], dims, preferred_element_type=jnp.float32
            )
            acc_up[...] += lax.dot_general(
                rows, up_buf[:, cols], dims, preferred_element_type=jnp.float32
            )
            return carry

        lax.fori_loop(0, width // deep, add, 0)
        gate_act = acc_gate[...]
        act = (gate_act / (1.0 + jnp.exp(-gate_act)) * acc_up[...]).astype(jnp.bfloat16)
        at = pl.ds(g * block, block)
        hidden[0, at, :] = act[:block]
        hidden[1 + 3 * core, at, :] = act[block:]
        handed.append(
            [
                send(hidden.at[0, at, :], hidden.at[3 - 2 * core, at, :], to_y),
                send(hidden.at[1 + 3 * core, at, :], hidden.at[2, at, :], to_t),
            ]
        )
        spare = pltpu.make_async_remote_copy(
            src_ref=hidden.at[4, at, :],
            dst_ref=hidden.at[3, at, :],
            send_sem=spare_send.at[g],
            recv_sem=spare_recv.at[g],
            device_id=to_d,
            device_id_type=MESH,
        )
        spares.append(spare)

        @pl.when(core == 1)
        def _():
            spare.start()

    hands = []

    def give(g, count, cols):
        span = pl.ds(2 * g, 2 * count)
        here = pl.ds(pl.multiple_of(e * GROUP, GROUP), GROUP)
        for i in range(2 * g, 2 * (g + count)):
            returned[i, here, cols] = produced[i, here, cols]
        return [
            send(
                produced.at[span, pl.ds(pl.multiple_of(peers[k] * GROUP, GROUP), GROUP), cols],
                returned.at[span, here, cols],
                {"expert": peers[k]},
            )
            for k in hops
        ]

    def project(g, first, count):
        here = pl.ds(g * block, block)

        def one(i, carry):
            at = pl.ds(pl.multiple_of(i * chunk, chunk), chunk)
            total = jnp.zeros((2 * block, chunk), jnp.float32)
            for pair in range(2):
                acts = hidden[pl.ds(2 * pair, 2), here, :].reshape(2 * block, 2 * units)
                total += jnp.dot(acts, down_buf[pair, :, at], preferred_element_type=jnp.float32)
            rows = total.astype(jnp.bfloat16)
            produced[g * 2, :, at] = rows[:block]
            produced[g * 2 + 1, :, at] = rows[block:]
            return carry

        lax.fori_loop(first, first + count, one, 0)

    beyond = e + 2 - 4 * ((e // 2) % 2)

    def key_rows_of(who):
        return pl.ds(pl.multiple_of((who % 4) * key_piece, key_piece), key_piece)

    key_copies = []

    def key_own():
        rows = key_rows_of(e)
        key_copies.append(send(key_ref.at[rows, :], key_buf.at[d % 2, rows, :], to_x))

    def key_pass(who, where):
        part = key_buf.at[dx % 2, key_rows_of(who), :]
        key_copies.append(send(part, part, where))

    def key_share():
        key_copies[0].wait_recv()
        key_pass(e, {"expert": beyond})
        key_pass(e, to_sibling)

    def key_relay():
        key_copies[1].wait_recv()
        key_pass(beyond, to_sibling)

    def collect(g):
        for copy in handed[g]:
            copy.wait_recv()

        @pl.when(core == 1)
        def _():
            spares[g].wait_recv()

    acc_keys[...] = jnp.zeros_like(acc_keys)
    squares[...] = jnp.zeros_like(squares)
    owners = (d, dy, dx, dd)
    tile_w, tile_t, key_sums = [], [], []

    def flag(owner, shard):
        return jnp.where(shard_ref[owner] == shard, 1.0, 0.0)

    def combine(c):
        for copy in hands[c]:
            copy.wait_recv()
        cols = pl.ds(c * chunk, chunk)
        for s in range(2):
            rows = jnp.concatenate([returned[2 * g + s, :, cols] for g in range(groups)], axis=0)
            branch = jnp.dot(mixing[s, 0], rows, preferred_element_type=jnp.float32)
            branch += jnp.dot(mixing[s, 1], rows, preferred_element_type=jnp.float32)
            base = tokens_ref[:, chunk_cols(d, c)] if s == 0 else tok_half[:, cols]
            tiles[s, :, cols] = (base.astype(jnp.float32) + branch).astype(jnp.bfloat16)
        tile_w.append(send(tiles.at[pl.ds(0, 2), :, cols], tiles.at[pl.ds(2, 2), :, cols], to_x))

    def keep(rows, at):
        student_ref[:, at] = rows.astype(jnp.bfloat16)
        squares[...] += jnp.sum(rows * rows, axis=-1, keepdims=True)

    def swap(c):
        tile_w[c].wait_recv()
        cols = pl.ds(c * chunk, chunk)
        stay = jnp.zeros((tok_dev, chunk), jnp.float32)
        leave = jnp.zeros((tok_dev, chunk), jnp.float32)
        for slot in range(4):
            rows = tiles[slot, :, cols].astype(jnp.float32)
            stay += flag(owners[slot], d) * rows
            leave += flag(owners[slot], dy) * rows
        passed[:, cols] = leave.astype(jnp.bfloat16)
        tile_t.append(send(passed.at[:, cols], far.at[:, cols], to_y))
        at = chunk_cols(d, c)
        gain = gain_ref[:, at]
        gained[:tok_dev, cols] = (stay * gain).astype(jnp.bfloat16)
        gained[tok_dev:, cols] = (leave * gain).astype(jnp.bfloat16)
        keep(stay, at)

    def finish(c):
        tile_t[c].wait_recv()
        keep(far[:, pl.ds(c * chunk, chunk)].astype(jnp.float32), chunk_cols(dy, c))

    def keys_of(c):
        acc_keys[...] += jnp.dot(
            gained[:, pl.ds(c * chunk, chunk)],
            key_buf[c // per_quarter, pl.ds((c % per_quarter) * chunk, chunk), :],
            preferred_element_type=jnp.float32,
        )

    early, others = [], []

    def push(g, p):
        if g == 0:
            down_here(p)
        elif p == 3:
            project(g, 0, CHUNKS)
            return
        elif p == 2:
            project(g, 0, CHUNKS)
            early.extend(give(g, 1, pl.ds(0, half)))
            return
        project(g, p * per_quarter, per_quarter)
        if p < 3:
            early.extend(give(g, 1, half_cols(p)))

    def last(p):
        for c in range(CHUNKS):
            project(groups - 1, c, 1)
            first = 1 if c >= p * per_quarter else groups - 1
            hands.append(give(first, groups - first, pl.ds(c * chunk, chunk)))

    def spread_rest():
        for ref, there in ((ids_ref, far_ids), (slots_ref, far_slots), (gates_ref, far_gates)):
            others.append(send(ref, there, to_y))
        for p in range(2):
            others.append(send(tokens_ref.at[:, quarter_cols(dy, p)], tok_half.at[:, half_cols(p)], to_y))

    table = {
        "Y": down_to_y,
        "X": down_to_x,
        "w": down_to_w,
        "t": down_to_t,
        "O": down_on,
        "F": forward,
        "W": pulled_in,
        "A": activate,
        "C": collect,
        "P": push,
        "L": last,
        "T": spread_rest,
        "K": key_own,
        "S": key_share,
    }
    for token in ORDER[ORDER.index("|") + 1 :]:
        table[token[0]](*[int(i) for i in token[1:]])
    for copy in others:
        copy.wait_recv()
    mix_into(1, far_ids, far_slots, far_gates)
    if len(key_copies) == 1:
        key_share()
    for copy in early:
        copy.wait_recv()
    own_key.wait()
    for c in range(CHUNKS + 2):
        if c < CHUNKS:
            combine(c)
        if c == CHUNKS:
            key_relay()
            for copy in key_copies[2:]:
                copy.wait_recv()
            for i in range(CHUNKS - 1):
                keys_of(i)
        if 0 <= c - 1 < CHUNKS:
            swap(c - 1)
        if 0 <= c - 2 < CHUNKS - 1:
            finish(c - 2)
    keys_of(CHUNKS - 1)
    part_width = key_width // 2
    for n in range(2):
        cols = pl.ds(n * part_width, part_width)
        key_part[0, :, cols] = acc_keys[tok_dev:, cols].astype(jnp.bfloat16)
        key_sums.append(send(key_part.at[0, :, cols], key_part.at[1, :, cols], to_y))
    finish(CHUNKS - 1)
    scale = lax.rsqrt(squares[...] / width + 1e-05)
    for n in range(2):
        cols = pl.ds(n * part_width, part_width)
        key_sums[n].wait_recv()
        total = acc_keys[:tok_dev, cols] + key_part[1, :, cols].astype(jnp.float32)
        keys_ref[:, cols] = (total * scale).astype(jnp.bfloat16)
    for copy in sent:
        copy.wait_send()

    @pl.when(core == 1)
    def _():
        for copy in spares:
            copy.wait_send()


def fused(
    tokens,
    gate_proj,
    up_proj,
    down_proj,
    route_ids,
    route_slots,
    route_gates,
    image_shard,
    norm_gain,
    key_proj,
    capacity,
):
    tok_dev, width = tokens.shape
    n_expert = lax.axis_size("expert")
    slots = n_expert * capacity
    groups = capacity // GROUP
    units = gate_proj.shape[1]
    half_width = width // 2
    key_rows, key_width = key_proj.shape
    remote = 14 + (n_expert - 1) * (4 * groups + CHUNKS) + 3 * groups + 5 + 2 * CHUNKS
    vmem = pl.BlockSpec(memory_space=pltpu.VMEM)
    anywhere = pl.BlockSpec(memory_space=pl.ANY)
    scalars = pl.BlockSpec(memory_space=pltpu.SMEM)
    half = jnp.bfloat16
    return pl.pallas_call(
        functools.partial(fused_kernel, n_expert, capacity),
        out_shape=(
            jax.ShapeDtypeStruct((tok_dev, width), half),
            jax.ShapeDtypeStruct((tok_dev, key_width), half),
        ),
        in_specs=[vmem] * 3 + [scalars] + [vmem] * 2 + [anywhere] * 4,
        out_specs=(vmem, vmem),
        scratch_shapes=[
            pltpu.VMEM((2 * units, width), half),
            pltpu.VMEM((2 * units, width), half),
            pltpu.VMEM((2, 2 * units, half_width), half),
            pltpu.VMEM((2, key_rows, key_width), half),
            pltpu.VMEM((slots, width), half),
            pltpu.VMEM((2 * slots, width), half),
            pltpu.VMEM((2 * groups, n_expert * GROUP, half_width), half),
            pltpu.VMEM((2 * groups, n_expert * GROUP, half_width), half),
            pltpu.VMEM((4, tok_dev, half_width), half),
            pltpu.VMEM((tok_dev, half_width), half),
            pltpu.VMEM((tok_dev, half_width), half),
            pltpu.VMEM((tok_dev, half_width), half),
            pltpu.VMEM((5, slots, 2 * units), half),
            pltpu.VMEM((2 * tok_dev, half_width), half),
            pltpu.VMEM((2, 2, tok_dev, slots), half),
            pltpu.VMEM((route_ids.shape[1], tok_dev), jnp.int32),
            pltpu.VMEM((route_ids.shape[1], tok_dev), jnp.int32),
            pltpu.VMEM((route_ids.shape[1], tok_dev), jnp.float32),
            pltpu.VMEM((2, tok_dev, key_width), half),
            pltpu.VMEM((2 * tok_dev, key_width), jnp.float32),
            pltpu.VMEM((2 * n_expert * GROUP, 2 * units), jnp.float32),
            pltpu.VMEM((2 * n_expert * GROUP, 2 * units), jnp.float32),
            pltpu.VMEM((tok_dev, 1), jnp.float32),
            pltpu.SemaphoreType.DMA((remote,)),
            pltpu.SemaphoreType.DMA((remote,)),
            pltpu.SemaphoreType.DMA((groups,)),
            pltpu.SemaphoreType.DMA((groups,)),
            pltpu.SemaphoreType.DMA((5,)),
        ],
        compiler_params=pltpu.CompilerParams(
            collective_id=0, has_side_effects=True, vmem_limit_bytes=60 * 1024 * 1024
        ),
    )(
        route_ids.T,
        route_slots.T,
        route_gates.T,
        image_shard.reshape(-1),
        norm_gain.reshape(1, -1),
        tokens,
        gate_proj,
        up_proj,
        down_proj,
        key_proj,
    )


def per_device(
    tokens,
    gate_proj,
    up_proj,
    down_proj,
    route_ids,
    route_slots,
    route_gates,
    image_shard,
    norm_gain,
    key_proj,
):
    tok_dev, model_width = tokens.shape
    top_count = route_ids.shape[1]
    experts = gate_proj.shape[0] * lax.axis_size("expert")
    capacity = 3 * tok_dev * top_count // (2 * experts)
    if capacity % 16 == 0 and gate_proj.shape[0] == 1 and lax.axis_size("dp") == 4 and experts % 4 == 0 and capacity >= 32:
        if tok_dev == IMG_TOK and gate_proj.shape[1] % 64 == 0 and key_proj.shape[0] % 512 == 0:
            return fused(
                tokens,
                gate_proj,
                up_proj,
                down_proj,
                route_ids,
                route_slots,
                route_gates,
                image_shard,
                norm_gain,
                key_proj,
                capacity,
            )
    slot_total = experts * capacity
    retained = route_slots < capacity
    slot_cells = jnp.where(retained, route_ids * capacity + route_slots, slot_total).reshape(-1)
    owners = jnp.arange(tok_dev * top_count, dtype=jnp.int32) // top_count
    cell_token = (
        jnp.full((slot_total + 1,), tok_dev, jnp.int32).at[slot_cells].set(owners)[:slot_total]
    )
    outgoing = jnp.take(tokens, cell_token, axis=0, mode="fill", fill_value=0).reshape(
        experts, capacity, model_width
    )
    arrived = lax.all_to_all(outgoing, "expert", split_axis=0, concat_axis=0, tiled=True)
    incoming = arrived.reshape(-1, model_width)
    hidden = activate(
        incoming,
        lax.all_gather(gate_proj, "dp", axis=1, tiled=True)[0],
        lax.all_gather(up_proj, "dp", axis=1, tiled=True)[0],
    )
    summed = jnp.dot(
        hidden,
        lax.all_gather(down_proj, "dp", axis=1, tiled=True)[0],
        preferred_element_type=jnp.float32,
    )
    produced = summed.astype(jnp.bfloat16).reshape(arrived.shape)
    returned = lax.all_to_all(produced, "expert", split_axis=0, concat_axis=0, tiled=True).reshape(
        -1, model_width
    )
    picked = jnp.take(returned, slot_cells, axis=0, mode="fill", fill_value=0).reshape(
        tok_dev, top_count, model_width
    )
    mixing = jnp.where(retained, route_gates, 0.0)
    branch = jnp.einsum("tk,tkd->td", mixing, picked.astype(jnp.float32))
    teacher = (tokens.astype(jnp.float32) + branch).astype(jnp.bfloat16)
    gathered = lax.all_gather(teacher, "dp", axis=0, tiled=True)
    shard_column = image_shard.reshape(-1)
    images_col = shard_column.shape[0]
    arrangement = jnp.argsort(shard_column * images_col + jnp.arange(images_col, dtype=jnp.int32))
    images = gathered.reshape(images_col, IMG_TOK, model_width)
    position = lax.axis_index("dp")
    ordered = jnp.take(images, arrangement, axis=0).reshape(images_col * IMG_TOK, model_width)
    student_rows = lax.dynamic_slice_in_dim(ordered, position * tok_dev, tok_dev, 0)
    normed = normalize(ordered, norm_gain)
    columns = lax.dynamic_slice_in_dim(normed, position * key_proj.shape[0], key_proj.shape[0], 1)
    projected = lax.psum_scatter(
        jnp.dot(columns, key_proj, preferred_element_type=jnp.float32),
        "dp",
        scatter_dimension=0,
        tiled=True,
    )
    return (student_rows, projected.astype(jnp.bfloat16))


def solution(mesh):
    in_specs = (
        P(("dp", "expert"), None),
        P("expert", "dp", None),
        P("expert", "dp", None),
        P("expert", "dp", None),
        P(("dp", "expert"), None),
        P(("dp", "expert"), None),
        P(("dp", "expert"), None),
        P(None, "expert"),
        P(),
        P("dp", None),
    )
    out_specs = (P(("dp", "expert"), None), P(("dp", "expert"), None))
    return jax.shard_map(
        per_device, mesh=mesh, in_specs=in_specs, out_specs=out_specs, check_vma=False
    )
```

```python
import functools

import jax
import jax.numpy as jnp
from jax import lax
from jax.experimental import pallas as pl
from jax.experimental.pallas import tpu as pltpu
from jax.sharding import PartitionSpec as P

IMG_TOK = 128


def normalize(values, norm_gain):
    wide = values.astype(jnp.float32)
    mean_square = jnp.mean(wide * wide, axis=-1, keepdims=True)
    return (wide * lax.rsqrt(mean_square + 1e-05) * norm_gain).astype(jnp.bfloat16)


def activate(incoming, gate_rows, up_rows):
    dims = (((1,), (1,)), ((), ()))
    gate_act = lax.dot_general(incoming, gate_rows, dims, preferred_element_type=jnp.float32)
    up_act = lax.dot_general(incoming, up_rows, dims, preferred_element_type=jnp.float32)
    return (jax.nn.silu(gate_act) * up_act).astype(jnp.bfloat16)


CHUNKS = 4
SHARE_AT = 1
ORDER = (
    "G", "w0", "w1", "|", "F0", "W", "t0", "t1", "A0", "O0", "O1", "F1", "C0", "P00", "F2", "P01", "A1", "C1", "P13", "P10", "A2", "T0", "T1", "K", "C2", "L0", "L1", "S",
)
GROUP = 16
MESH = pl.DeviceIdType.MESH


def fused_kernel(
    n_expert,
    capacity,
    ids_ref,
    slots_ref,
    gates_ref,
    shard_ref,
    gain_ref,
    tokens_ref,
    gate_ref,
    up_ref,
    down_ref,
    key_ref,
    student_ref,
    keys_ref,
    gate_buf,
    up_buf,
    down_buf,
    key_buf,
    outgoing,
    incoming,
    produced,
    returned,
    tiles,
    passed,
    far,
    tok_half,
    hidden,
    gained,
    mixing,
    far_ids,
    far_slots,
    far_gates,
    key_part,
    student,
    keys,
    acc_keys,
    acc_gate,
    acc_up,
    squares,
    send_sem,
    recv_sem,
    spare_send,
    spare_recv,
    local_sem,
):
    d = lax.axis_index("dp")
    e = lax.axis_index("expert")
    dx = d + 1 - 2 * (d % 2)
    dy = (d + 2) % 4
    dd = (dx + 2) % 4
    core = e % 2
    sibling = e + 1 - 2 * core
    w = dx + core * (dy - dx)
    t = dy + core * (dx - dy)
    tok_dev, width = tokens_ref.shape
    units = gate_ref.shape[1]
    half = width // 2
    quarter_width = width // 4
    chunk = half // CHUNKS
    per_quarter = CHUNKS // 2
    key_rows, key_width = key_ref.shape
    key_piece = key_rows // 4
    slots = n_expert * capacity
    groups = capacity // GROUP
    block = n_expert * GROUP
    counts = {"remote": 0, "local": 0}
    sent = []

    def send(source, target, where, go=True):
        index = counts["remote"]
        counts["remote"] += 1
        copy = pltpu.make_async_remote_copy(
            src_ref=source,
            dst_ref=target,
            send_sem=send_sem.at[index],
            recv_sem=recv_sem.at[index],
            device_id=where,
            device_id_type=MESH,
        )
        if go:
            copy.start()
        sent.append(copy)
        return copy

    def local(source, target):
        index = counts["local"]
        counts["local"] += 1
        copy = pltpu.make_async_copy(source, target, local_sem.at[index])
        copy.start()
        return copy

    to_x, to_y, to_sibling = {"dp": dx}, {"dp": dy}, {"expert": sibling}
    to_w, to_t = {"dp": w}, {"dp": t}
    hops = sorted(range(1, n_expert), key=lambda k: -min(k, n_expert - k))
    peers = {k: lax.rem(e + k, n_expert) for k in hops}
    senders = {k: lax.rem(e + n_expert - k, n_expert) for k in hops}

    def quarter_of(owner, p):
        return (owner // 2) * 2 + p

    def unit_rows(owner):
        place = owner % 2 + core * (owner // 2 - owner % 2)
        return pl.ds(pl.multiple_of(place * units, units), units)

    def quarter_cols(owner, p):
        return pl.ds(pl.multiple_of(quarter_of(owner, p) * quarter_width, quarter_width), quarter_width)

    def chunk_cols(owner, c):
        first = quarter_of(owner, c // per_quarter) * quarter_width + (c % per_quarter) * chunk
        return pl.ds(pl.multiple_of(first, chunk), chunk)

    def group_rows(g, who):
        return pl.ds(pl.multiple_of(g * block + who * GROUP, GROUP), GROUP)

    def incoming_rows(g, s, who):
        return pl.ds(pl.multiple_of((g * 2 + s) * block + who * GROUP, GROUP), GROUP)

    barrier = pltpu.get_barrier_semaphore()
    for where in [to_x, to_y, {"dp": dd}] + [{"expert": peers[k]} for k in hops]:
        pl.semaphore_signal(barrier, inc=1, device_id=where, device_id_type=MESH)

    step = 512

    def routes(ids, queues):
        grid = lax.broadcasted_iota(jnp.int32, (slots, tok_dev), 0)
        hits = []
        for k in range(ids.shape[0]):
            queue = queues[k : k + 1, :]
            place = lax.div(queue, GROUP) * block + ids[k : k + 1, :] * GROUP + lax.rem(queue, GROUP)
            hits.append(grid == jnp.where(queue < capacity, place, slots))
        return hits

    def mix_into(s, ids, queues, weights):
        mix = jnp.zeros((slots, tok_dev), jnp.float32)
        for k, hit in enumerate(routes(ids, queues)):
            mix += jnp.where(hit, weights[k : k + 1, :], 0.0)
        turned = mix.T
        mix_hi = turned.astype(jnp.bfloat16)
        mixing[s, 0] = mix_hi
        mixing[s, 1] = (turned - mix_hi.astype(jnp.float32)).astype(jnp.bfloat16)

    named = jnp.zeros((slots, tok_dev), jnp.float32)
    for hit in routes(ids_ref, slots_ref):
        named += jnp.where(hit, 1.0, 0.0)
    spread = named.astype(jnp.bfloat16)

    def fill_group(g):
        chosen = spread[g * block : (g + 1) * block, :]

        def fill(i, carry):
            cols = pl.ds(pl.multiple_of(i * step, step), step)
            rows = jnp.dot(chosen, tokens_ref[:, cols], preferred_element_type=jnp.float32)
            outgoing[pl.ds(g * block, block), cols] = rows.astype(jnp.bfloat16)
            return carry

        lax.fori_loop(0, width // step, fill, 0)

    fill_group(0)
    pl.semaphore_wait(barrier, n_expert + 2)

    mine = unit_rows(d)
    down_x, down_y, down_f, own_down = [], [], [], []

    def half_cols(p):
        return pl.ds(p * quarter_width, quarter_width)

    for p in range(2):
        part = down_ref.at[0, :, quarter_cols(dy, p)]
        down_y.append(send(part, down_buf.at[1 - core, mine, half_cols(p)], to_y, False))
        part = down_ref.at[0, :, quarter_cols(d, p)]
        down_x.append(send(part, down_buf.at[core, mine, half_cols(p)], to_x, False))

    def down_to_y(p):
        down_y[p].start()

    def down_to_x(p):
        down_x[p].start()

    def down_to_w(p):
        @pl.when(core == 0)
        def _():
            down_x[p].start()

        @pl.when(core == 1)
        def _():
            down_y[p].start()

    def down_to_t(p):
        @pl.when(core == 0)
        def _():
            down_y[p].start()

        @pl.when(core == 1)
        def _():
            down_x[p].start()

    def down_on(p):
        down_y[p].wait_recv()
        part = down_buf.at[1 - core, unit_rows(dy), half_cols(p)]
        down_f.append(send(part, down_buf.at[1, unit_rows(dy), half_cols(p)], to_x))

    def down_here(p):
        own_down[p].wait()
        down_x[p].wait_recv()
        down_f[p].wait_recv()

    pulled = []

    def pull():
        pulled.append(send(gate_ref.at[0], gate_buf.at[mine, :], to_w))
        pulled.append(send(up_ref.at[0], up_buf.at[mine, :], to_w))

    def pulled_in():
        own_gate.wait()
        own_up.wait()
        for copy in pulled:
            copy.wait_recv()

    own_gate = local(gate_ref.at[0], gate_buf.at[mine, :])
    own_up = local(up_ref.at[0], up_buf.at[mine, :])
    for p in range(2):
        own_down.append(local(down_ref.at[0, :, quarter_cols(d, p)], down_buf.at[0, mine, half_cols(p)]))
    own_key = local(key_ref, key_buf.at[d % 2])

    for token in ORDER[: ORDER.index("|")]:
        {"G": pull, "Y": down_to_y, "X": down_to_x, "w": down_to_w, "t": down_to_t}[token[0]](*[int(i) for i in token[1:]])
    dispatched, forwarded = [], []
    for g in range(groups):
        if g:
            fill_group(g)
        dispatched.append(
            {
                k: send(
                    outgoing.at[group_rows(g, peers[k]), :],
                    incoming.at[incoming_rows(g, 0, e), :],
                    {"expert": peers[k]},
                )
                for k in hops
            }
        )
        forwarded.append(
            [send(outgoing.at[group_rows(g, e), :], incoming.at[incoming_rows(g, 1, e), :], to_t)]
        )
        incoming[incoming_rows(g, 0, e), :] = outgoing[group_rows(g, e), :]

    mix_into(0, ids_ref, slots_ref, gates_ref)

    def forward(g):
        for k in hops:
            dispatched[g][k].wait_recv()
            forwarded[g].append(
                send(
                    incoming.at[incoming_rows(g, 0, senders[k]), :],
                    incoming.at[incoming_rows(g, 1, senders[k]), :],
                    to_t,
                )
            )

    dims = (((1,), (1,)), ((), ()))
    deep = 1024
    handed, spares = [], []

    def activate(g):
        for copy in forwarded[g]:
            copy.wait_recv()
        here = pl.ds(g * 2 * block, 2 * block)
        acc_gate[...] = jnp.zeros_like(acc_gate)
        acc_up[...] = jnp.zeros_like(acc_up)

        def add(i, carry):
            cols = pl.ds(pl.multiple_of(i * deep, deep), deep)
            rows = incoming[here, cols]
            acc_gate[...] += lax.dot_general(
                rows, gate_buf[:, cols], dims, preferred_element_type=jnp.float32
            )
            acc_up[...] += lax.dot_general(
                rows, up_buf[:, cols], dims, preferred_element_type=jnp.float32
            )
            return carry

        lax.fori_loop(0, width // deep, add, 0)
        gate_act = acc_gate[...]
        act = (gate_act / (1.0 + jnp.exp(-gate_act)) * acc_up[...]).astype(jnp.bfloat16)
        at = pl.ds(g * block, block)
        hidden[0, at, :] = act[:block]
        hidden[1 + 3 * core, at, :] = act[block:]
        handed.append(
            [
                send(hidden.at[0, at, :], hidden.at[3 - 2 * core, at, :], to_y),
                send(hidden.at[1 + 3 * core, at, :], hidden.at[2, at, :], to_t),
            ]
        )
        spare = pltpu.make_async_remote_copy(
            src_ref=hidden.at[4, at, :],
            dst_ref=hidden.at[3, at, :],
            send_sem=spare_send.at[g],
            recv_sem=spare_recv.at[g],
            device_id={"dp": dd},
            device_id_type=MESH,
        )
        spares.append(spare)

        @pl.when(core == 1)
        def _():
            spare.start()

    hands = []

    def give(g, count, cols):
        span = pl.ds(2 * g, 2 * count)
        here = pl.ds(pl.multiple_of(e * GROUP, GROUP), GROUP)
        for i in range(2 * g, 2 * (g + count)):
            returned[i, here, cols] = produced[i, here, cols]
        return [
            send(
                produced.at[span, pl.ds(pl.multiple_of(peers[k] * GROUP, GROUP), GROUP), cols],
                returned.at[span, here, cols],
                {"expert": peers[k]},
            )
            for k in hops
        ]

    def project(g, first, count):
        here = pl.ds(g * block, block)

        def one(i, carry):
            at = pl.ds(pl.multiple_of(i * chunk, chunk), chunk)
            total = jnp.zeros((2 * block, chunk), jnp.float32)
            for pair in range(2):
                acts = hidden[pl.ds(2 * pair, 2), here, :].reshape(2 * block, 2 * units)
                total += jnp.dot(acts, down_buf[pair, :, at], preferred_element_type=jnp.float32)
            rows = total.astype(jnp.bfloat16)
            produced[g * 2, :, at] = rows[:block]
            produced[g * 2 + 1, :, at] = rows[block:]
            return carry

        lax.fori_loop(first, first + count, one, 0)

    beyond = e + 2 - 4 * ((e // 2) % 2)

    def key_rows_of(who):
        return pl.ds(pl.multiple_of((who % 4) * key_piece, key_piece), key_piece)

    key_copies = []

    def key_own():
        rows = key_rows_of(e)
        key_copies.append(send(key_ref.at[rows, :], key_buf.at[d % 2, rows, :], to_x))

    def key_pass(who, where):
        part = key_buf.at[dx % 2, key_rows_of(who), :]
        key_copies.append(send(part, part, where))

    def key_share():
        key_copies[0].wait_recv()
        key_pass(e, {"expert": beyond})
        key_pass(e, to_sibling)

    def key_relay():
        key_copies[1].wait_recv()
        key_pass(beyond, to_sibling)

    def collect(g):
        for copy in handed[g]:
            copy.wait_recv()

        @pl.when(core == 1)
        def _():
            spares[g].wait_recv()

    acc_keys[...] = jnp.zeros_like(acc_keys)
    squares[...] = jnp.zeros_like(squares)
    owners = (d, dy, dx, dd)
    tile_w, tile_t, key_sums = [], [], []

    def flag(owner, shard):
        return jnp.where(shard_ref[owner] == shard, 1.0, 0.0)

    def combine(c):
        for copy in hands[c]:
            copy.wait_recv()
        cols = pl.ds(c * chunk, chunk)
        for s in range(2):
            rows = jnp.concatenate([returned[2 * g + s, :, cols] for g in range(groups)], axis=0)
            branch = jnp.dot(mixing[s, 0], rows, preferred_element_type=jnp.float32)
            branch += jnp.dot(mixing[s, 1], rows, preferred_element_type=jnp.float32)
            base = tokens_ref[:, chunk_cols(d, c)] if s == 0 else tok_half[:, cols]
            tiles[s, :, cols] = (base.astype(jnp.float32) + branch).astype(jnp.bfloat16)
        tile_w.append(send(tiles.at[pl.ds(0, 2), :, cols], tiles.at[pl.ds(2, 2), :, cols], to_x))

    written = []

    def keep(rows, at):
        student[:, at] = rows.astype(jnp.bfloat16)
        written.append(local(student.at[:, at], student_ref.at[:, at]))
        squares[...] += jnp.sum(rows * rows, axis=-1, keepdims=True)

    def swap(c):
        tile_w[c].wait_recv()
        cols = pl.ds(c * chunk, chunk)
        stay = jnp.zeros((tok_dev, chunk), jnp.float32)
        leave = jnp.zeros((tok_dev, chunk), jnp.float32)
        for slot in range(4):
            rows = tiles[slot, :, cols].astype(jnp.float32)
            stay += flag(owners[slot], d) * rows
            leave += flag(owners[slot], dy) * rows
        passed[:, cols] = leave.astype(jnp.bfloat16)
        tile_t.append(send(passed.at[:, cols], far.at[:, cols], to_y))
        at = chunk_cols(d, c)
        gain = gain_ref[:, at]
        gained[:tok_dev, cols] = (stay * gain).astype(jnp.bfloat16)
        gained[tok_dev:, cols] = (leave * gain).astype(jnp.bfloat16)
        keep(stay, at)

    def finish(c):
        tile_t[c].wait_recv()
        keep(far[:, pl.ds(c * chunk, chunk)].astype(jnp.float32), chunk_cols(dy, c))

    def keys_of(c):
        acc_keys[...] += jnp.dot(
            gained[:, pl.ds(c * chunk, chunk)],
            key_buf[c // per_quarter, pl.ds((c % per_quarter) * chunk, chunk), :],
            preferred_element_type=jnp.float32,
        )

    early, others = [], []

    def push(g, p):
        if g == 0:
            down_here(p)
        elif p == 3:
            project(g, 0, CHUNKS)
            return
        elif p == 2:
            project(g, 0, CHUNKS)
            early.extend(give(g, 1, pl.ds(0, half)))
            return
        project(g, p * per_quarter, per_quarter)
        if p < 3:
            early.extend(give(g, 1, half_cols(p)))

    def last(p):
        for c in range(p * per_quarter, (p + 1) * per_quarter):
            project(groups - 1, c, 1)
            first = 1 if p else groups - 1
            hands.append(give(first, groups - first, pl.ds(c * chunk, chunk)))

    def early_in():
        for copy in early:
            copy.wait_recv()
        early.clear()

    for ref, there in ((ids_ref, far_ids), (slots_ref, far_slots), (gates_ref, far_gates)):
        others.append(send(ref, there, to_y, False))
    for p in range(2):
        part = tokens_ref.at[:, quarter_cols(dy, p)]
        others.append(send(part, tok_half.at[:, half_cols(p)], to_y, False))

    def spread_rest(which):
        @pl.when(core == which)
        def _():
            for copy in others:
                copy.start()

    table = {
        "Y": down_to_y,
        "X": down_to_x,
        "w": down_to_w,
        "t": down_to_t,
        "O": down_on,
        "F": forward,
        "W": pulled_in,
        "A": activate,
        "C": collect,
        "P": push,
        "L": last,
        "E": early_in,
        "T": spread_rest,
        "K": key_own,
        "S": key_share,
    }
    for token in ORDER[ORDER.index("|") + 1 :]:
        table[token[0]](*[int(i) for i in token[1:]])
    for copy in others:
        copy.wait_recv()
    mix_into(1, far_ids, far_slots, far_gates)
    if not key_copies:
        key_own()
    early_in()
    own_key.wait()
    for c in range(CHUNKS + 2):
        if c < CHUNKS:
            combine(c)
        if c == CHUNKS:
            key_relay()
            for copy in key_copies[2:]:
                copy.wait_recv()
            for i in range(CHUNKS - 1):
                keys_of(i)
        if c == SHARE_AT and len(key_copies) == 1:
            key_share()
        if 0 <= c - 1 < CHUNKS:
            swap(c - 1)
        if 0 <= c - 2 < CHUNKS - 1:
            finish(c - 2)
    keys_of(CHUNKS - 1)
    part_width = key_width // 2
    for n in range(2):
        cols = pl.ds(n * part_width, part_width)
        key_part[0, :, cols] = acc_keys[tok_dev:, cols].astype(jnp.bfloat16)
        key_sums.append(send(key_part.at[0, :, cols], key_part.at[1, :, cols], to_y))
    finish(CHUNKS - 1)
    for copy in sent[:-2]:
        copy.wait_send()

    @pl.when(core == 1)
    def _():
        for copy in spares:
            copy.wait_send()

    scale = lax.rsqrt(squares[...] / width + 1e-05)
    for n in range(2):
        cols = pl.ds(n * part_width, part_width)
        key_sums[n].wait_recv()
        total = acc_keys[:tok_dev, cols] + key_part[1, :, cols].astype(jnp.float32)
        keys[:, cols] = (total * scale).astype(jnp.bfloat16)
        written.append(local(keys.at[:, cols], keys_ref.at[:, cols]))
    for copy in sent[-2:]:
        copy.wait_send()
    for copy in written:
        copy.wait()


def fused(
    tokens,
    gate_proj,
    up_proj,
    down_proj,
    route_ids,
    route_slots,
    route_gates,
    image_shard,
    norm_gain,
    key_proj,
    capacity,
):
    tok_dev, width = tokens.shape
    n_expert = lax.axis_size("expert")
    slots = n_expert * capacity
    groups = capacity // GROUP
    units = gate_proj.shape[1]
    half_width = width // 2
    key_rows, key_width = key_proj.shape
    remote = 14 + (n_expert - 1) * (4 * groups + CHUNKS) + 3 * groups + 5 + 2 * CHUNKS
    vmem = pl.BlockSpec(memory_space=pltpu.VMEM)
    anywhere = pl.BlockSpec(memory_space=pl.ANY)
    scalars = pl.BlockSpec(memory_space=pltpu.SMEM)
    half = jnp.bfloat16
    return pl.pallas_call(
        functools.partial(fused_kernel, n_expert, capacity),
        out_shape=(
            jax.ShapeDtypeStruct((tok_dev, width), half),
            jax.ShapeDtypeStruct((tok_dev, key_width), half),
        ),
        in_specs=[vmem] * 3 + [scalars] + [vmem] * 2 + [anywhere] * 4,
        out_specs=(anywhere, anywhere),
        scratch_shapes=[
            pltpu.VMEM((2 * units, width), half),
            pltpu.VMEM((2 * units, width), half),
            pltpu.VMEM((2, 2 * units, half_width), half),
            pltpu.VMEM((2, key_rows, key_width), half),
            pltpu.VMEM((slots, width), half),
            pltpu.VMEM((2 * slots, width), half),
            pltpu.VMEM((2 * groups, n_expert * GROUP, half_width), half),
            pltpu.VMEM((2 * groups, n_expert * GROUP, half_width), half),
            pltpu.VMEM((4, tok_dev, half_width), half),
            pltpu.VMEM((tok_dev, half_width), half),
            pltpu.VMEM((tok_dev, half_width), half),
            pltpu.VMEM((tok_dev, half_width), half),
            pltpu.VMEM((5, slots, 2 * units), half),
            pltpu.VMEM((2 * tok_dev, half_width), half),
            pltpu.VMEM((2, 2, tok_dev, slots), half),
            pltpu.VMEM((route_ids.shape[1], tok_dev), jnp.int32),
            pltpu.VMEM((route_ids.shape[1], tok_dev), jnp.int32),
            pltpu.VMEM((route_ids.shape[1], tok_dev), jnp.float32),
            pltpu.VMEM((2, tok_dev, key_width), half),
            pltpu.VMEM((tok_dev, width), half),
            pltpu.VMEM((tok_dev, key_width), half),
            pltpu.VMEM((2 * tok_dev, key_width), jnp.float32),
            pltpu.VMEM((2 * n_expert * GROUP, 2 * units), jnp.float32),
            pltpu.VMEM((2 * n_expert * GROUP, 2 * units), jnp.float32),
            pltpu.VMEM((tok_dev, 1), jnp.float32),
            pltpu.SemaphoreType.DMA((remote,)),
            pltpu.SemaphoreType.DMA((remote,)),
            pltpu.SemaphoreType.DMA((groups,)),
            pltpu.SemaphoreType.DMA((groups,)),
            pltpu.SemaphoreType.DMA((5 + 2 * CHUNKS + 2,)),
        ],
        compiler_params=pltpu.CompilerParams(
            collective_id=0, has_side_effects=True, vmem_limit_bytes=60 * 1024 * 1024
        ),
    )(
        route_ids.T,
        route_slots.T,
        route_gates.T,
        image_shard.reshape(-1),
        norm_gain.reshape(1, -1),
        tokens,
        gate_proj,
        up_proj,
        down_proj,
        key_proj,
    )


def per_device(
    tokens,
    gate_proj,
    up_proj,
    down_proj,
    route_ids,
    route_slots,
    route_gates,
    image_shard,
    norm_gain,
    key_proj,
):
    tok_dev, model_width = tokens.shape
    top_count = route_ids.shape[1]
    experts = gate_proj.shape[0] * lax.axis_size("expert")
    capacity = 3 * tok_dev * top_count // (2 * experts)
    if capacity % 16 == 0 and gate_proj.shape[0] == 1 and lax.axis_size("dp") == 4 and experts % 4 == 0 and capacity >= 32:
        if tok_dev == IMG_TOK and gate_proj.shape[1] % 64 == 0 and key_proj.shape[0] % 512 == 0:
            return fused(
                tokens,
                gate_proj,
                up_proj,
                down_proj,
                route_ids,
                route_slots,
                route_gates,
                image_shard,
                norm_gain,
                key_proj,
                capacity,
            )
    slot_total = experts * capacity
    retained = route_slots < capacity
    slot_cells = jnp.where(retained, route_ids * capacity + route_slots, slot_total).reshape(-1)
    owners = jnp.arange(tok_dev * top_count, dtype=jnp.int32) // top_count
    cell_token = (
        jnp.full((slot_total + 1,), tok_dev, jnp.int32).at[slot_cells].set(owners)[:slot_total]
    )
    outgoing = jnp.take(tokens, cell_token, axis=0, mode="fill", fill_value=0).reshape(
        experts, capacity, model_width
    )
    arrived = lax.all_to_all(outgoing, "expert", split_axis=0, concat_axis=0, tiled=True)
    incoming = arrived.reshape(-1, model_width)
    hidden = activate(
        incoming,
        lax.all_gather(gate_proj, "dp", axis=1, tiled=True)[0],
        lax.all_gather(up_proj, "dp", axis=1, tiled=True)[0],
    )
    summed = jnp.dot(
        hidden,
        lax.all_gather(down_proj, "dp", axis=1, tiled=True)[0],
        preferred_element_type=jnp.float32,
    )
    produced = summed.astype(jnp.bfloat16).reshape(arrived.shape)
    returned = lax.all_to_all(produced, "expert", split_axis=0, concat_axis=0, tiled=True).reshape(
        -1, model_width
    )
    picked = jnp.take(returned, slot_cells, axis=0, mode="fill", fill_value=0).reshape(
        tok_dev, top_count, model_width
    )
    mixing = jnp.where(retained, route_gates, 0.0)
    branch = jnp.einsum("tk,tkd->td", mixing, picked.astype(jnp.float32))
    teacher = (tokens.astype(jnp.float32) + branch).astype(jnp.bfloat16)
    gathered = lax.all_gather(teacher, "dp", axis=0, tiled=True)
    shard_column = image_shard.reshape(-1)
    images_col = shard_column.shape[0]
    arrangement = jnp.argsort(shard_column * images_col + jnp.arange(images_col, dtype=jnp.int32))
    images = gathered.reshape(images_col, IMG_TOK, model_width)
    position = lax.axis_index("dp")
    ordered = jnp.take(images, arrangement, axis=0).reshape(images_col * IMG_TOK, model_width)
    student_rows = lax.dynamic_slice_in_dim(ordered, position * tok_dev, tok_dev, 0)
    normed = normalize(ordered, norm_gain)
    columns = lax.dynamic_slice_in_dim(normed, position * key_proj.shape[0], key_proj.shape[0], 1)
    projected = lax.psum_scatter(
        jnp.dot(columns, key_proj, preferred_element_type=jnp.float32),
        "dp",
        scatter_dimension=0,
        tiled=True,
    )
    return (student_rows, projected.astype(jnp.bfloat16))


def solution(mesh):
    in_specs = (
        P(("dp", "expert"), None),
        P("expert", "dp", None),
        P("expert", "dp", None),
        P("expert", "dp", None),
        P(("dp", "expert"), None),
        P(("dp", "expert"), None),
        P(("dp", "expert"), None),
        P(None, "expert"),
        P(),
        P("dp", None),
    )
    out_specs = (P(("dp", "expert"), None), P(("dp", "expert"), None))
    return jax.shard_map(
        per_device, mesh=mesh, in_specs=in_specs, out_specs=out_specs, check_vma=False
    )
```
